32 devices in a mesh: batch: 2 (over x), rows: 4 (over z), chan: 4 (over y, core).
Axes of the slice: x: 2, y: 2, z: 4, core: 2. Of those that a mesh axis runs over, the one named last changes fastest.
Arguments:
- images: float32 [16, 24, 16, 32], P('batch', None, ('rows', 'chan')), may hold values from -6 to 6
- shift_mid: float32 [3, 24], replicated, may hold values from -1.75 to 1.75
- gain_mid: float32 [3, 24], replicated, may hold values from -0.3 to 0.3
- lower_mid: float32 [3, 24, 24], replicated, may hold values from -1.25 to 1.25
- upper_mid: float32 [3, 24, 24], replicated, may hold values from -1.25 to 1.25
- diag_mid: float32 [3, 24], replicated, may hold values from -0.3 to 0.3
- first_mid: bfloat16 [3, 9, 12, 512], replicated, may hold values from -0.625 to 0.625
- first_bias_mid: bfloat16 [3, 512], replicated, may hold values from -3 to 3
- second_mid: bfloat16 [3, 512, 512], replicated, may hold values from -0.25 to 0.25
- second_bias_mid: float32 [3, 512], replicated, may hold values from -3 to 3
- third_mid: bfloat16 [3, 9, 512, 24], replicated, may hold values from -0.09375 to 0.09375
- third_bias_mid: float32 [3, 24], replicated, may hold values from -3 to 3
- shift_top: float32 [2, 48], replicated, may hold values from -1.75 to 1.75
- gain_top: float32 [2, 48], replicated, may hold values from -0.3 to 0.3
- lower_top: float32 [2, 48, 48], replicated, may hold values from -0.875 to 0.875
- upper_top: float32 [2, 48, 48], replicated, may hold values from -0.875 to 0.875
- diag_top: float32 [2, 48], replicated, may hold values from -0.3 to 0.3
- first_top: bfloat16 [2, 9, 24, 512], replicated, may hold values from -0.4375 to 0.4375
- first_bias_top: bfloat16 [2, 512], replicated, may hold values from -3 to 3
- second_top: bfloat16 [2, 512, 512], replicated, may hold values from -0.25 to 0.25
- second_bias_top: float32 [2, 512], replicated, may hold values from -3 to 3
- third_top: bfloat16 [2, 9, 512, 48], replicated, may hold values from -0.09375 to 0.09375
- third_bias_top: float32 [2, 48], replicated, may hold values from -3 to 3
Outputs:
- latent_mid: float32 [16, 12, 16, 32], P('batch', None, ('rows', 'chan'))
- latent_top: float32 [16, 48, 8, 16], P(('batch', 'chan'), None, 'rows')
- loglik: float32 [16], P(('batch', 'chan'))
The draws below stay inside these ranges and needn't reach their ends.
All inputs are finite; a program needn't handle non-finite values.
Results may differ from the reference program's by a relative error of at most 0.008.
Values may be sent and summed in bfloat16 or wider, within the bound.
A program may use at most 64 MiB of HBM per device.

```python
import math
import jax
import jax.numpy as jnp
from jax import lax

HID = 512
C2 = 24
W2 = 32
STEPS2 = 3
STEPS3 = 2
B = 16
H2 = 16
C3 = 48


def level_of(rng, extent, split, least, high):
    gain, own = 1.0, jax.random.fold_in(rng, 6)
    for axis_at, shards_of in split:
        draws = jnp.exp(jax.random.uniform(jax.random.fold_in(own, axis_at), (shards_of,), jnp.float32, least / len(split), high / len(split)))
        gain = gain * jnp.repeat(draws, extent[axis_at] // shards_of).reshape([-1 if axis == axis_at else 1 for axis in range(len(extent))])
    return gain


def centred(rng, dims, width, bound, shards=(), held_as=jnp.bfloat16):
    array = width * jax.random.normal(rng, dims, jnp.float32)
    if shards:
        array = array * level_of(rng, dims, shards, -0.22, 0.18)
    return jnp.clip(array, -bound, bound).astype(held_as)


def setup_inputs(seed: int = 0) -> dict:
    keys = jax.random.split(jax.random.key(seed), 24)
    return {
        "images": centred(keys[0], (B, C2, H2, W2), 1.0, 6.0, ((0, 2), (2, 16)), jnp.float32),
        "shift_mid": centred(keys[1], (STEPS2, C2), 0.3, 1.75, (), jnp.float32),
        "gain_mid": jnp.clip(jax.random.uniform(keys[2], (STEPS2, C2), jnp.float32, -0.3, 0.3), -0.3, 0.3),
        "lower_mid": centred(keys[3], (STEPS2, C2, C2), C2 ** -0.5, 1.25, (), jnp.float32),
        "upper_mid": centred(keys[4], (STEPS2, C2, C2), C2 ** -0.5, 1.25, (), jnp.float32),
        "diag_mid": jnp.clip(jax.random.uniform(keys[5], (STEPS2, C2), jnp.float32, -0.3, 0.3), -0.3, 0.3),
        "first_mid": centred(keys[6], (STEPS2, 9, C2 // 2, HID), (9 * C2 // 2) ** -0.5, 0.625),
        "first_bias_mid": centred(keys[7], (STEPS2, HID), 0.5, 3.0),
        "second_mid": centred(keys[8], (STEPS2, HID, HID), HID ** -0.5, 0.25),
        "second_bias_mid": centred(keys[9], (STEPS2, HID), 0.5, 3.0, (), jnp.float32),
        "third_mid": centred(keys[10], (STEPS2, 9, HID, C2), (9 * HID) ** -0.5, 0.09375),
        "third_bias_mid": centred(keys[11], (STEPS2, C2), 0.5, 3.0, (), jnp.float32),
        "shift_top": centred(keys[12], (STEPS3, C3), 0.3, 1.75, (), jnp.float32),
        "gain_top": jnp.clip(jax.random.uniform(keys[13], (STEPS3, C3), jnp.float32, -0.3, 0.3), -0.3, 0.3),
        "lower_top": centred(keys[14], (STEPS3, C3, C3), C3 ** -0.5, 0.875, (), jnp.float32),
        "upper_top": centred(keys[15], (STEPS3, C3, C3), C3 ** -0.5, 0.875, (), jnp.float32),
        "diag_top": jnp.clip(jax.random.uniform(keys[16], (STEPS3, C3), jnp.float32, -0.3, 0.3), -0.3, 0.3),
        "first_top": centred(keys[17], (STEPS3, 9, C2, HID), (9 * C2) ** -0.5, 0.4375),
        "first_bias_top": centred(keys[18], (STEPS3, HID), 0.5, 3.0),
        "second_top": centred(keys[19], (STEPS3, HID, HID), HID ** -0.5, 0.25),
        "second_bias_top": centred(keys[20], (STEPS3, HID), 0.5, 3.0, (), jnp.float32),
        "third_top": centred(keys[21], (STEPS3, 9, HID, C3), (9 * HID) ** -0.5, 0.09375),
        "third_bias_top": centred(keys[22], (STEPS3, C3), 0.5, 3.0, (), jnp.float32),
    }


log_two_pi = math.log(2.0 * math.pi)


def spatial_conv(source, weights):
    height = source.shape[1]
    columns = source.shape[2]
    padded = jnp.pad(source, ((0, 0), (1, 1), (1, 1))).astype(jnp.float32)
    summed = jnp.zeros((weights.shape[2], height, columns), jnp.float32)
    for tap_idx in range(9):
        row_off = tap_idx // 3
        col_off = tap_idx % 3
        window = padded[:, row_off:row_off + height, col_off:col_off + columns]
        summed = summed + jnp.einsum('chw,co->ohw', window, weights[tap_idx].astype(jnp.float32))
    return summed


def flow_step(flow_state, params):
    shift_vec, gain_vec, lower_raw, upper_raw, diag_log, first_w, first_b, second_w, second_b, third_w, third_b = params
    channels = flow_state.shape[0]
    half_chan = channels // 2
    cell_count = flow_state.shape[1] * flow_state.shape[2]
    mixed_state = (flow_state + shift_vec[:, None, None]) * jnp.exp(gain_vec)[:, None, None]
    lower_mat = jnp.tril(lower_raw, -1) + jnp.eye(channels, dtype=jnp.float32)
    upper_mat = jnp.triu(upper_raw, 1) + jnp.diag(jnp.exp(diag_log))
    matrix = jnp.dot(lower_mat, upper_mat, precision=lax.Precision.HIGHEST)
    mixed_state = jnp.einsum('oc,chw->ohw', matrix, mixed_state, precision=lax.Precision.HIGHEST)
    part_a = mixed_state[:half_chan]
    part_b = mixed_state[half_chan:]
    coupled = part_a.astype(jnp.bfloat16)
    inner = jax.nn.relu(spatial_conv(coupled, first_w) + first_b.astype(jnp.float32)[:, None, None]).astype(jnp.bfloat16)
    middle = jnp.einsum('chw,co->ohw', inner.astype(jnp.float32), second_w.astype(jnp.float32))
    middle = jax.nn.relu(middle + second_b[:, None, None]).astype(jnp.bfloat16)
    output = spatial_conv(middle, third_w) + third_b[:, None, None]
    gate_pre = output[:half_chan] + 2.0
    updated = (part_b + output[half_chan:]) * jax.nn.sigmoid(gate_pre)
    step_term = cell_count * (jnp.sum(gain_vec) + jnp.sum(diag_log)) + jnp.sum(jax.nn.log_sigmoid(gate_pre))
    return jnp.concatenate([part_a, updated], axis=0), step_term


def image_flow(picture, params_mid, params_top):
    flow_state = picture
    logdet = jnp.zeros((), jnp.float32)
    for step_num in range(params_mid[0].shape[0]):
        flow_state, step_term = flow_step(flow_state, tuple(p[step_num] for p in params_mid))
        logdet = logdet + step_term
    half_chan = flow_state.shape[0] // 2
    latent_mid = flow_state[:half_chan]
    kept_chan = flow_state[half_chan:]
    count_chan, height, columns = kept_chan.shape
    squeezed = kept_chan.reshape(count_chan, height // 2, 2, columns // 2, 2).transpose(0, 2, 4, 1, 3)
    flow_state = squeezed.reshape(count_chan * 4, height // 2, columns // 2)
    for step_num in range(params_top[0].shape[0]):
        flow_state, step_term = flow_step(flow_state, tuple(p[step_num] for p in params_top))
        logdet = logdet + step_term
    latent_top = flow_state
    latent_count = latent_mid.size + latent_top.size
    logprob = -0.5 * (jnp.sum(latent_mid * latent_mid) + jnp.sum(latent_top * latent_top)) - 0.5 * log_two_pi * latent_count
    total_dims = picture.shape[0] * picture.shape[1] * picture.shape[2]
    return latent_mid, latent_top, (logprob + logdet) / total_dims


def reference(images, shift_mid, gain_mid, lower_mid, upper_mid, diag_mid, first_mid, first_bias_mid, second_mid, second_bias_mid, third_mid, third_bias_mid, shift_top, gain_top, lower_top, upper_top, diag_top, first_top, first_bias_top, second_top, second_bias_top, third_top, third_bias_top):
    params_mid = (shift_mid, gain_mid, lower_mid, upper_mid, diag_mid, first_mid, first_bias_mid, second_mid, second_bias_mid, third_mid, third_bias_mid)
    params_top = (shift_top, gain_top, lower_top, upper_top, diag_top, first_top, first_bias_top, second_top, second_bias_top, third_top, third_bias_top)
    latent_mid, latent_top, loglik = lax.map(lambda picture: image_flow(picture, params_mid, params_top), images)
    return (latent_mid, latent_top, loglik)
```

```python
import functools
import math

import jax
import jax.numpy as jnp
from jax import lax
from jax.experimental import pallas as pl
from jax.experimental.pallas import tpu as pltpu
from jax.sharding import PartitionSpec as P

MESH = pl.DeviceIdType.MESH
LANES = 128
CHUNK = 512
FINE = lax.Precision.HIGHEST
log_two_pi = math.log(2.0 * math.pi)
f32 = jnp.float32
bf16 = jnp.bfloat16


def up8(n):
    return -(-n // 8) * 8


def iota(shape, dim):
    return lax.broadcasted_iota(jnp.int32, shape, dim)


def dot_nt(a, b, precision=None):
    return lax.dot_general(
        a, b, (((1,), (1,)), ((), ())), preferred_element_type=f32, precision=precision
    )


def dot_tn(a, b):
    return lax.dot_general(a, b, (((0,), (0,)), ((), ())), preferred_element_type=f32)


def roll_back(x, amount):
    n = x.shape[1]
    amount = amount % n
    return x if amount == 0 else pltpu.roll(x, n - amount, 1)


def neighbour_masks(n, height, width):
    lane = iota((1, n), 1)
    place = lax.rem(lane, height * width)
    row = lax.div(place, width)
    col = lax.rem(place, width)
    row_ok = {-1: row >= 1, 1: row < height - 1}
    col_ok = {-1: col >= 1, 1: col < width - 1}
    return row_ok, col_ok


def keep(x, ok):
    return jnp.where(ok, x, 0.0)


def spread_taps(q, masks, width):
    row_ok, col_ok = masks
    by_col = {}
    for dc in (-1, 0, 1):
        by_col[dc] = q if dc == 0 else keep(roll_back(q, dc), col_ok[dc])
    taps = []
    for dr in (-1, 0, 1):
        for dc in (-1, 0, 1):
            x = by_col[dc]
            taps.append(x if dr == 0 else keep(roll_back(x, dr * width), row_ok[dr]))
    return jnp.concatenate(taps, axis=0)


def gather_taps(y_ref, channels, n, masks, width):
    row_ok, col_ok = masks
    total = None
    for dc in (-1, 0, 1):
        part = None
        for dr in (-1, 0, 1):
            tap = (dr + 1) * 3 + dc + 1
            y = y_ref[tap * channels : (tap + 1) * channels, :n]
            if dr != 0:
                y = keep(roll_back(y, dr * width), row_ok[dr])
            part = y if part is None else part + y
        if dc != 0:
            part = keep(roll_back(part, dc), col_ok[dc])
        total = part if total is None else total + part
    return total


def mixing(lower, upper, diag_row, gain_row, shift_row, in_map):
    channels = lower.shape[0]
    half = channels // 2
    padded = up8(half)
    i = iota((channels, channels), 0)
    j = iota((channels, channels), 1)
    eye = jnp.where(i == j, 1.0, 0.0)
    low = jnp.where(i > j, lower, 0.0) + eye
    upp = (jnp.where(i < j, upper, 0.0) + eye * jnp.exp(diag_row)) * jnp.exp(gain_row)
    out_map = pad_map(channels)
    rows = jnp.dot(out_map, low, precision=FINE, preferred_element_type=f32)
    mat = jnp.dot(rows, upp, precision=FINE, preferred_element_type=f32)
    bias = jnp.sum(mat * shift_row, axis=1, keepdims=True)
    if in_map is not None:
        mat = dot_nt(mat, in_map, FINE)
    return mat, bias


def pad_map(channels):
    half = channels // 2
    padded = up8(half)
    i = iota((2 * padded, channels), 0)
    j = iota((2 * padded, channels), 1)
    first = (j < half) & (i == j)
    second = (j >= half) & (i - padded == j - half)
    return jnp.where(first | second, 1.0, 0.0)


def squeeze_map(kept, padded):
    i = iota((4 * padded, 4 * kept), 0)
    j = iota((4 * padded, 4 * kept), 1)
    same = (lax.rem(i, padded) == lax.div(j, 4)) & (lax.div(i, padded) == lax.rem(j, 4))
    return jnp.where(same, 1.0, 0.0)


def to_column(row):
    n = row.shape[1]
    eye = iota((n, n), 0) == iota((n, n), 1)
    return jnp.sum(jnp.where(eye, row, 0.0), axis=1, keepdims=True)


def kernel(dims, *refs):
    n_rows, n_chan, split, height, width, places, count = dims
    sources, refs = refs[: len(places)], refs[len(places) :]
    (mid_out, top_out, lik_out), refs = refs[:3], refs[3:]
    held, refs = refs[:count], refs[count:]
    (
        images,
        vecs_mid,
        vecs_top,
        mats_in_mid,
        mats_in_top,
        w1_raw,
        first_bias_mid,
        first_bias_top,
        second_bias_mid,
        second_bias_top,
        w2_all,
        w13_all,
    ) = held
    (
        outbox,
        inbox,
        w1_mid,
        pick,
        y_scr,
        z_scr,
        z_send,
        z_recv,
        t_send,
        t_recv,
        t_scr,
        w_sem,
        sems,
    ) = refs
    send_sem, recv_sem, z_send_sem, z_recv_sem, t_send_sem, t_recv_sem = [
        sems.at[k] for k in range(6)
    ]
    n_imgs, channels, block = images.shape
    steps_mid = vecs_mid.shape[1]
    steps_top = vecs_top.shape[1]
    group = n_imgs // n_chan
    peers = n_rows * n_chan
    b = lax.axis_index("batch")
    r = lax.axis_index("rows")
    c = lax.axis_index("chan")
    me = r * n_chan + c
    mine = lax.rem(r, split)
    base = r - mine
    own_imgs = group // split
    swap = split > 1 and n_chan % 2 == 0

    def paired(chan):
        return chan + 1 - 2 * lax.rem(chan, 2) if swap else chan

    work = paired(c)

    def device(row, chan):
        return {"batch": b, "rows": row, "chan": chan}

    def fetch(at):
        where, offset, extent = places[at]
        target = held[where] if offset is None else held[where].at[offset]
        if extent is not None:
            target = held[where].at[pl.ds(offset, extent)]
        pltpu.make_async_copy(sources[at], target, w_sem.at[where]).start()

    def arrive(where):
        pltpu.make_async_copy(held[where], held[where], w_sem.at[where]).wait()

    def drain(ref, total, send, recv):
        return pltpu.make_async_remote_copy(
            src_ref=ref.at[pl.ds(0, total)],
            dst_ref=ref.at[pl.ds(0, total)],
            send_sem=send,
            recv_sem=recv,
            device_id=device(r, c),
            device_id_type=MESH,
        )

    fetch(0)
    barrier = pltpu.get_barrier_semaphore()
    for d in range(1, peers):
        other = lax.rem(me + d, peers)
        pl.semaphore_signal(
            barrier,
            inc=1,
            device_id=device(other // n_chan, lax.rem(other, n_chan)),
            device_id_type=MESH,
        )

    for at in range(1, len(places)):
        fetch(at)
    arrive(0)

    per = LANES // block
    slabs = channels // 8
    pieces = [(img, slab) for img in range(own_imgs) for slab in range(slabs)]
    packs = -(-len(pieces) // per)
    for dest in range(n_chan * split):
        rows = []
        for pack in range(packs):
            parts = []
            for img, slab in pieces[pack * per : (pack + 1) * per]:
                parts.append(images[dest * own_imgs + img, slab * 8 : slab * 8 + 8, :])
            while len(parts) < per:
                parts.append(jnp.zeros((8, block), f32))
            rows.append(jnp.concatenate(parts, axis=1))
        outbox[dest] = jnp.concatenate(rows, axis=0).astype(bf16)

    pl.semaphore_wait(barrier, peers - 1)
    for d in range(1, peers):
        other = lax.rem(me + d, peers)
        other_chan = lax.rem(other, n_chan)
        copy = pltpu.make_async_remote_copy(
            src_ref=outbox.at[paired(other_chan) * split + lax.rem(other // n_chan, split)],
            dst_ref=inbox.at[me],
            send_sem=send_sem,
            recv_sem=recv_sem,
            device_id=device(other // n_chan, other_chan),
            device_id_type=MESH,
        )
        copy.start()

    inbox[me] = outbox[work * split + mine]

    for where in range(1, count):
        arrive(where)
    shift_mid, gain_mid, diag_mid, third_bias_mid = [vecs_mid[k] for k in range(4)]
    shift_top, gain_top, diag_top, third_bias_top = [vecs_top[k] for k in range(4)]
    lower_mid, upper_mid = mats_in_mid.at[0], mats_in_mid.at[1]
    lower_top, upper_top = mats_in_top.at[0], mats_in_top.at[1]
    deep = w13_all.shape[1]
    w3_mid = [w13_all.at[s] for s in range(steps_mid)]
    w1_top = [w13_all.at[steps_mid + s] for s in range(steps_top)]
    w3_top = [
        w13_all.at[pl.ds(steps_mid + steps_top + 2 * s, 2)] for s in range(steps_top)
    ]
    half = channels // 2
    padded = up8(half)
    top_channels = 4 * half
    mats_mid = []
    for s in range(steps_mid):
        mats_mid.append(
            mixing(
                lower_mid[s],
                upper_mid[s],
                diag_mid[s : s + 1, :],
                gain_mid[s : s + 1, :],
                shift_mid[s : s + 1, :],
                None if s == 0 else pad_map(channels),
            )
        )
    mats_top = []
    for s in range(steps_top):
        mats_top.append(
            mixing(
                lower_top[s],
                upper_top[s],
                diag_top[s : s + 1, :],
                gain_top[s : s + 1, :],
                shift_top[s : s + 1, :],
                squeeze_map(half, padded) if s == 0 else pad_map(top_channels),
            )
        )
    bias3_mid = [to_column(third_bias_mid[s : s + 1, :]) for s in range(steps_mid)]
    bias3_top = [to_column(third_bias_top[s : s + 1, :]) for s in range(steps_top)]
    span = pick.shape[0]
    quarter = span // 4
    to = iota((1, span), 1)
    ij = lax.div(to, quarter)
    cell = lax.rem(to, quarter)
    coarse_w = width // 2
    origin = (2 * lax.div(cell, coarse_w) + lax.div(ij, 2)) * width
    origin = origin + 2 * lax.rem(cell, coarse_w) + lax.rem(ij, 2)
    for k in range(0, span, LANES):
        pick[k : k + LANES, :] = jnp.where(
            iota((LANES, span), 0) + k == origin, 1.0, 0.0
        ).astype(bf16)
    for s in range(steps_mid):
        for tap in range(9):
            w = w1_raw[s, tap].astype(f32)
            if padded > half:
                w = jnp.concatenate([w, jnp.zeros((padded - half, w.shape[1]), f32)], axis=0)
            w1_mid[s, tap * padded : (tap + 1) * padded, :] = w.astype(bf16)
    const_mid = height * width * (jnp.sum(gain_mid) + jnp.sum(diag_mid))
    const_top = (height // 2) * (width // 2) * (jnp.sum(gain_top) + jnp.sum(diag_top))

    if peers > 1:
        drain(inbox, peers - 1, send_sem, recv_sem).wait_recv()

    cells = height * width
    n_mid = own_imgs * cells
    columns = []
    letters = [inbox[source].astype(f32) for source in range(peers)]
    for img in range(own_imgs):
        for quad in range(peers // per):
            stack = []
            for slab in range(slabs):
                at = img * slabs + slab
                lo = (at % per) * block
                top = at // per * 8
                parts = [
                    letters[quad * per + j][top : top + 8, lo : lo + block] for j in range(per)
                ]
                stack.append(jnp.concatenate(parts, axis=1))
            columns.append(jnp.concatenate(stack, axis=0))
    state = jnp.concatenate(columns, axis=1)

    strip = n_chan * block
    team = split * n_chan
    seat = mine * n_chan + c

    def share(ua):
        z_scr[...] = ua
        for to_row in range(split):
            for img in range(own_imgs):
                begin = pl.multiple_of(img * cells + (base + to_row) * strip, LANES)
                z_send[to_row, img] = z_scr[:, pl.ds(begin, strip)].astype(bf16)
        for d in range(1, team):
            other = lax.rem(seat + d, team)
            copy = pltpu.make_async_remote_copy(
                src_ref=z_send.at[other // n_chan],
                dst_ref=z_recv.at[seat],
                send_sem=z_send_sem,
                recv_sem=z_recv_sem,
                device_id=device(base + other // n_chan, lax.rem(other, n_chan)),
                device_id_type=MESH,
            )
            copy.start()
        z_recv[seat] = z_send[mine]

    def step(state, mat, bias, w1, b1, w2, b2, w3, b3, masks, width, chans, last=False):
        n = state.shape[1]
        half_c = chans // 2
        hp = up8(half_c)
        u = jnp.dot(mat, state, precision=FINE, preferred_element_type=f32) + bias
        ua, ub = u[:hp], u[hp:]
        if last:
            share(ua)
        spread = spread_taps(ua, masks, width).astype(bf16)
        size = min(CHUNK, n)
        for at in range(0, n, size):
            h1 = dot_tn(spread[:, at : at + size], w1)
            h1 = jnp.maximum(h1 + b1, 0.0).astype(bf16)
            h2 = jnp.dot(h1, w2[...], preferred_element_type=f32)
            h2 = jnp.maximum(h2 + b2, 0.0).astype(bf16)
            w3_now = w3[...].reshape(9 * chans, -1)
            y_scr[: 9 * chans, at : at + size] = dot_nt(w3_now, h2)
        out = gather_taps(y_scr, chans, n, masks, width) + b3
        g = out[:hp] + 2.0
        t = out[half_c:]
        if hp > half_c:
            t = jnp.concatenate([t, jnp.zeros((hp - half_c, n), f32)], axis=0)
        e = jnp.exp(-jnp.abs(g))
        inv = 1.0 / (1.0 + e)
        gate = jnp.where(g >= 0, inv, e * inv)
        logs = jnp.minimum(g, 0.0) - jnp.log(1.0 + e)
        if hp > half_c:
            logs = jnp.where(iota((hp, n), 0) < half_c, logs, 0.0)
        return ua, (ub + t) * gate, logs

    masks = neighbour_masks(n_mid, height, width)
    score = None
    for s in range(steps_mid):
        ua, updated, logs = step(
            state,
            *mats_mid[s],
            w1_mid[s],
            first_bias_mid[s : s + 1, :].astype(f32),
            w2_all.at[s],
            second_bias_mid[s : s + 1, :],
            w3_mid[s],
            bias3_mid[s],
            masks,
            width,
            channels,
            s == steps_mid - 1,
        )
        score = logs if score is None else score + logs
        if s < steps_mid - 1:
            state = jnp.concatenate([ua, updated], axis=0)
    score = score - 0.5 * ua * ua

    parts = []
    rest = updated
    for _ in range(3):
        piece = rest.astype(bf16)
        rest = rest - piece.astype(f32)
        parts.append(piece)
    blocks = []
    parts = jnp.concatenate([x.astype(f32) for x in parts], axis=0).astype(bf16)
    for at in range(0, n_mid, span):
        got = jnp.dot(parts[:, at : at + span], pick[...], preferred_element_type=f32)
        total = got[:padded] + got[padded : 2 * padded] + got[2 * padded :]
        blocks.append(
            jnp.concatenate([total[:, k * quarter : (k + 1) * quarter] for k in range(4)], axis=0)
        )
    state = jnp.concatenate(blocks, axis=1)

    n_top = n_mid // 4
    masks = neighbour_masks(n_top, height // 2, width // 2)
    score_top = None
    for s in range(steps_top):
        ua, updated, logs = step(
            state,
            *mats_top[s],
            w1_top[s][...],
            first_bias_top[s : s + 1, :].astype(f32),
            w2_all.at[steps_mid + s],
            second_bias_top[s : s + 1, :],
            w3_top[s],
            bias3_top[s],
            masks,
            width // 2,
            top_channels,
        )
        score_top = logs if score_top is None else score_top + logs
        state = jnp.concatenate([ua, updated], axis=0)
    score_top = score_top - 0.5 * (ua * ua + updated * updated)

    top_cells = cells // 4
    own = top_cells // n_rows
    hp = up8(top_channels // 2)
    if hp * 2 > top_channels:
        state = jnp.concatenate([ua[: top_channels // 2], updated[: top_channels // 2]], axis=0)
    fixed = const_mid + const_top - 0.5 * log_two_pi * (half * cells + top_channels * top_cells)
    high = t_send.shape[2]
    folds = -(-top_channels // high)
    if folds * high > top_channels:
        filler = jnp.zeros((folds * high - top_channels, n_top), f32)
        state = jnp.concatenate([state, filler], axis=0)
    t_scr[...] = state
    for img in range(own_imgs):
        total = jnp.sum(score[:, img * cells : (img + 1) * cells])
        total = total + jnp.sum(score_top[:, img * top_cells : (img + 1) * top_cells])
        lik = jnp.full((high, own), (total + fixed) / (channels * cells), f32)
        coarse = lik.astype(bf16).astype(f32)
        lik = jnp.where(iota((high, own), 0) == 0, coarse, lik - coarse)
        for to_row in range(split):
            at = img * top_cells + (base + to_row) * own
            window = t_scr[:, img * top_cells : (img + 1) * top_cells]
            parts = []
            for row in range(n_rows):
                piece = window[:, row * own : (row + 1) * own]
                parts.append(
                    jnp.concatenate(
                        [piece[k * high : (k + 1) * high] for k in range(folds)] + [lik], axis=1
                    )
                )
            chosen = parts[to_row]
            for start in range(split, n_rows, split):
                chosen = jnp.where(base == start, parts[start + to_row], chosen)
            t_send[to_row, img] = chosen.astype(bf16)
    t_count = split if swap else split - 1
    for d in range(split - t_count, split):
        other = lax.rem(mine + d, split)
        copy = pltpu.make_async_remote_copy(
            src_ref=t_send.at[other],
            dst_ref=t_recv.at[mine],
            send_sem=t_send_sem,
            recv_sem=t_recv_sem,
            device_id=device(base + other, work),
            device_id_type=MESH,
        )
        copy.start()
    if not swap:
        t_recv[mine] = t_send[mine]

    if team > 1:
        drain(z_recv, team - 1, z_send_sem, z_recv_sem).wait_recv()
    for here in range(n_chan):

        @pl.when(c == here)
        def _():
            for source in range(n_chan):
                holder = source + 1 - 2 * (source % 2) if swap else source
                for img in range(group):
                    sender = img // own_imgs * n_chan + holder
                    at = (source * group + img) * half
                    mid_out[at : at + half, :] = z_recv[sender, img % own_imgs].astype(f32)[
                        :half, here * block : (here + 1) * block
                    ]

    if peers > 1:
        drain(inbox, peers - 1, send_sem, recv_sem).wait_send()
    if team > 1:
        drain(z_recv, team - 1, z_send_sem, z_recv_sem).wait_send()
    if t_count > 0:
        drain(t_recv, t_count, t_send_sem, t_recv_sem).wait()
    liks = []
    letters = []
    for img in range(group):
        letter = t_recv[img // own_imgs, img % own_imgs].astype(f32)
        letters.append(letter)
        lik = letter[:2, folds * own : folds * own + 1]
        liks.append(lik[:1] + lik[1:])
    flipped = jnp.transpose(jnp.concatenate(letters, axis=0))
    for img in range(group):
        for k in range(folds):
            size = min(high, top_channels - k * high)
            top_out[img, :, k * high : k * high + size] = flipped[
                k * own : (k + 1) * own, img * high : img * high + size
            ]
    lik_out[...] = jnp.concatenate(liks, axis=1)


def deliver(*refs):
    count = len(refs) // 2
    sems = refs[-1]
    copies = [
        pltpu.make_async_copy(refs[at], refs[count + at], sems.at[at]) for at in range(count)
    ]
    for copy in copies:
        copy.start()
    for copy in copies:
        copy.wait()


def body(sizes, images, *params):
    (
        shift_mid,
        gain_mid,
        lower_mid,
        upper_mid,
        diag_mid,
        first_mid,
        first_bias_mid,
        second_mid,
        second_bias_mid,
        third_mid,
        third_bias_mid,
        shift_top,
        gain_top,
        lower_top,
        upper_top,
        diag_top,
        first_top,
        first_bias_top,
        second_top,
        second_bias_top,
        third_top,
        third_bias_top,
    ) = params
    n_rows, n_chan = sizes
    n_imgs, channels, own_rows, width = images.shape
    peers = n_rows * n_chan
    height = own_rows * peers
    block = own_rows * width
    group = n_imgs // n_chan
    half = channels // 2
    padded = up8(half)
    steps_mid, hidden = first_bias_mid.shape
    steps_top, top_channels = shift_top.shape
    cells = height * width
    split = group if n_rows % group == 0 else 1
    own_imgs = group // split
    n_mid = own_imgs * cells
    span = 4 * LANES
    packs = -(-(own_imgs * (channels // 8)) * block // LANES)
    strip = n_chan * block
    own = cells // 4 // n_rows
    high = -(-top_channels // max(1, LANES // own - 1) // 16) * 16
    folds = -(-top_channels // high)

    deep = 9 * channels
    w1_top = first_top.reshape(steps_top, deep, hidden)
    w3_mid = third_mid.transpose(0, 1, 3, 2).reshape(steps_mid, deep, hidden)
    w3_top = third_top.transpose(0, 1, 3, 2).reshape(2 * steps_top, deep, hidden)
    layout = (
        ((images.reshape(n_imgs, channels, block), None),),
        tuple((x, k) for k, x in enumerate((shift_mid, gain_mid, diag_mid, third_bias_mid))),
        tuple((x, k) for k, x in enumerate((shift_top, gain_top, diag_top, third_bias_top))),
        ((lower_mid, 0), (upper_mid, 1)),
        ((lower_top, 0), (upper_top, 1)),
        ((first_mid, None),),
        ((first_bias_mid, None),),
        ((first_bias_top, None),),
        ((second_bias_mid, None),),
        ((second_bias_top, None),),
        ((second_mid, 0), (second_top, steps_mid)),
        ((w3_mid, 0), (w1_top, steps_mid), (w3_top, steps_mid + steps_top)),
    )
    operands, places, stores = [], [], []
    for where, entry in enumerate(layout):
        first = entry[0][0]
        joined = where >= len(layout) - 2
        if joined:
            shape = (sum(x.shape[0] for x, _ in entry),) + first.shape[1:]
        elif entry[0][1] is None:
            shape = first.shape
        else:
            shape = (len(entry),) + first.shape
        stores.append(pltpu.VMEM(shape, first.dtype))
        for x, offset in entry:
            operands.append(x)
            places.append((where, offset, x.shape[0] if joined else None))
    vmem = pl.BlockSpec(memory_space=pltpu.VMEM)
    hbm = pl.BlockSpec(memory_space=pl.ANY)
    count = len(stores)
    results = [
        (n_imgs * half, block),
        (group, own, top_channels),
        (1, group),
    ]
    held = pl.pallas_call(
        functools.partial(kernel, (n_rows, n_chan, split, height, width, places, count)),
        out_shape=[pltpu.VMEM(x, f32) for x in results],
        in_specs=[hbm] * len(operands),
        out_specs=[vmem] * len(results),
        scratch_shapes=stores
        + [
            pltpu.VMEM((n_chan * split, packs * 8, LANES), bf16),
            pltpu.VMEM((peers, packs * 8, LANES), bf16),
            pltpu.VMEM((steps_mid, 9 * padded, hidden), bf16),
            pltpu.VMEM((span, span), bf16),
            pltpu.VMEM((9 * top_channels, n_mid), f32),
            pltpu.VMEM((padded, n_mid), f32),
            pltpu.VMEM((split, own_imgs, padded, strip), bf16),
            pltpu.VMEM((split * n_chan, own_imgs, padded, strip), bf16),
            pltpu.VMEM((split, own_imgs, high, (folds + 1) * own), bf16),
            pltpu.VMEM((split, own_imgs, high, (folds + 1) * own), bf16),
            pltpu.VMEM((folds * high, n_mid // 4), f32),
            pltpu.SemaphoreType.DMA((count,)),
            pltpu.SemaphoreType.DMA((6,)),
        ],
        compiler_params=pltpu.CompilerParams(
            collective_id=0, has_side_effects=True, vmem_limit_bytes=56 * 1024 * 1024
        ),
        name="flow",
    )(*operands)
    mid, top, lik = pl.pallas_call(
        deliver,
        out_shape=[jax.ShapeDtypeStruct(x, f32) for x in results],
        in_specs=[vmem] * len(results),
        out_specs=[hbm] * len(results),
        scratch_shapes=[pltpu.SemaphoreType.DMA((len(results),))],
        name="deliver",
    )(*[pltpu.with_memory_space_constraint(x, pltpu.VMEM) for x in held])
    latent_mid = mid.reshape(n_imgs, half, own_rows, width)
    latent_top = top.reshape(group, -1, width // 2, top_channels).transpose(0, 3, 1, 2)
    return latent_mid, latent_top, lik.reshape(group)


def solution(mesh):
    sizes = (mesh.shape["rows"], mesh.shape["chan"])
    placed = (P("batch", None, ("rows", "chan"), None),) + (P(),) * 22
    return jax.shard_map(
        functools.partial(body, sizes),
        mesh=mesh,
        in_specs=placed,
        out_specs=(
            P("batch", None, ("rows", "chan"), None),
            P(("batch", "chan"), None, "rows", None),
            P(("batch", "chan")),
        ),
        check_vma=False,
    )
```

```python
import functools
import math

import jax
import jax.numpy as jnp
from jax import lax
from jax.experimental import pallas as pl
from jax.experimental.pallas import tpu as pltpu
from jax.sharding import PartitionSpec as P

MESH = pl.DeviceIdType.MESH
LANES = 128
CHUNK = 512
FINE = lax.Precision.HIGHEST
log_two_pi = math.log(2.0 * math.pi)
f32 = jnp.float32
bf16 = jnp.bfloat16


def up8(n):
    return -(-n // 8) * 8


def iota(shape, dim):
    return lax.broadcasted_iota(jnp.int32, shape, dim)


def dot_nt(a, b, precision=None):
    return lax.dot_general(
        a, b, (((1,), (1,)), ((), ())), preferred_element_type=f32, precision=precision
    )


def dot_tn(a, b):
    return lax.dot_general(a, b, (((0,), (0,)), ((), ())), preferred_element_type=f32)


def roll_back(x, amount):
    n = x.shape[1]
    amount = amount % n
    return x if amount == 0 else pltpu.roll(x, n - amount, 1)


def keep(x, ok):
    return jnp.where(ok, x, 0.0)


def tiles_of(x):
    return [x[:, at : at + LANES] for at in range(0, x.shape[1], LANES)]


def join(parts):
    return parts[0] if len(parts) == 1 else jnp.concatenate(parts, axis=1)


def shift_cols(x, dc, width):
    if dc == 0:
        return x
    col = lax.rem(iota((1, LANES), 1), width)
    ok = col < width - 1 if dc > 0 else col >= 1
    return join([keep(roll_back(tile, dc), ok) for tile in tiles_of(x)])


def shift_rows(x, dr, width, cells):
    if dr == 0:
        return x
    strip = lax.div(iota((1, LANES), 1), width)
    ok = strip < LANES // width - 1 if dr > 0 else strip >= 1
    moved = []
    for at in range(0, x.shape[1], cells):
        tiles = tiles_of(x[:, at : at + cells])
        edge = tiles[0] if dr > 0 else tiles[-1]
        edge = keep(roll_back(edge, dr * width), ok)
        moved += tiles[1:] + [edge] if dr > 0 else [edge] + tiles[:-1]
    return join(moved)


def by_row(x, width, cells):
    depth = cells // LANES
    if depth == 1:
        return x
    parts = []
    for at in range(0, x.shape[1], cells):
        for row in range(cells // width):
            lo = at + row % depth * LANES + row // depth * width
            parts.append(x[:, lo : lo + width])
    return join(parts)


def spread_taps(q, width, cells):
    by_col = {dc: shift_cols(q, dc, width) for dc in (-1, 0, 1)}
    taps = []
    for dr in (-1, 0, 1):
        for dc in (-1, 0, 1):
            taps.append(shift_rows(by_col[dc], dr, width, cells))
    return jnp.concatenate(taps, axis=0)


def gather_taps(y_ref, channels, n, width, cells):
    total = None
    for dc in (-1, 0, 1):
        part = None
        for dr in (-1, 0, 1):
            tap = (dr + 1) * 3 + dc + 1
            y = y_ref[tap * channels : (tap + 1) * channels, :n]
            y = shift_rows(y, dr, width, cells)
            part = y if part is None else part + y
        part = shift_cols(part, dc, width)
        total = part if total is None else total + part
    return total


def mixing(table, lower, upper, diag_row, gain_row, shift_row, in_map):
    channels = lower.shape[0]
    half = channels // 2
    padded = up8(half)
    i = iota((channels, channels), 0)
    j = iota((channels, channels), 1)
    eye = jnp.where(i == j, 1.0, 0.0)
    low = jnp.where(i > j, lower, 0.0) + eye
    upp = (jnp.where(i < j, upper, 0.0) + eye * jnp.exp(diag_row)) * jnp.exp(gain_row)
    out_map = pad_map(channels)
    rows = jnp.dot(out_map, low, precision=FINE, preferred_element_type=f32)
    mat = jnp.dot(rows, upp, precision=FINE, preferred_element_type=f32)
    bias = jnp.sum(mat * shift_row, axis=1, keepdims=True)
    for j in range(channels):
        table[j] = jnp.broadcast_to(mat[:padded, j : j + 1], (padded, LANES))
    table[channels] = jnp.broadcast_to(bias[:padded], (padded, LANES))
    mat, bias = mat[padded:], bias[padded:]
    if in_map is not None:
        mat = dot_nt(mat, in_map, FINE)
    return mat, bias


def pad_map(channels):
    half = channels // 2
    padded = up8(half)
    i = iota((2 * padded, channels), 0)
    j = iota((2 * padded, channels), 1)
    first = (j < half) & (i == j)
    second = (j >= half) & (i - padded == j - half)
    return jnp.where(first | second, 1.0, 0.0)


def squeeze_map(kept, padded):
    i = iota((4 * padded, 4 * kept), 0)
    j = iota((4 * padded, 4 * kept), 1)
    same = (lax.rem(i, padded) == lax.div(j, 4)) & (lax.div(i, padded) == lax.rem(j, 4))
    return jnp.where(same, 1.0, 0.0)


def to_column(row):
    n = row.shape[1]
    eye = iota((n, n), 0) == iota((n, n), 1)
    return jnp.sum(jnp.where(eye, row, 0.0), axis=1, keepdims=True)


def kernel(dims, *refs):
    n_rows, n_chan, split, height, width, places, count = dims
    sources, refs = refs[: len(places)], refs[len(places) :]
    (mid_out, top_out, lik_out), refs = refs[:3], refs[3:]
    held, refs = refs[:count], refs[count:]
    (
        images,
        vecs_mid,
        vecs_top,
        mats_in_mid,
        mats_in_top,
        w1_raw,
        first_bias_mid,
        first_bias_top,
        second_bias_mid,
        second_bias_top,
        w2_all,
        w13_all,
    ) = held
    (
        outbox,
        inbox,
        w1_mid,
        mix_mid,
        mix_top,
        s_mid,
        s_top,
        y_scr,
        z_scr,
        z_send,
        z_recv,
        t_send,
        t_recv,
        t_scr,
        w_sem,
        sems,
    ) = refs
    send_sem, recv_sem, z_send_sem, z_recv_sem, t_send_sem, t_recv_sem = [
        sems.at[k] for k in range(6)
    ]
    n_imgs, channels, block = images.shape
    steps_mid = vecs_mid.shape[1]
    steps_top = vecs_top.shape[1]
    group = n_imgs // n_chan
    peers = n_rows * n_chan
    b = lax.axis_index("batch")
    r = lax.axis_index("rows")
    c = lax.axis_index("chan")
    me = r * n_chan + c
    mine = lax.rem(r, split)
    base = r - mine
    own_imgs = group // split
    swap = split > 1 and n_chan % 2 == 0

    def paired(chan):
        return chan + 1 - 2 * lax.rem(chan, 2) if swap else chan

    work = paired(c)

    def device(row, chan):
        return {"batch": b, "rows": row, "chan": chan}

    def fetch(at):
        where, offset, extent = places[at]
        target = held[where] if offset is None else held[where].at[offset]
        if extent is not None:
            target = held[where].at[pl.ds(offset, extent)]
        pltpu.make_async_copy(sources[at], target, w_sem.at[where]).start()

    def arrive(where):
        pltpu.make_async_copy(held[where], held[where], w_sem.at[where]).wait()

    def drain(ref, total, send, recv):
        return pltpu.make_async_remote_copy(
            src_ref=ref.at[pl.ds(0, total)],
            dst_ref=ref.at[pl.ds(0, total)],
            send_sem=send,
            recv_sem=recv,
            device_id=device(r, c),
            device_id_type=MESH,
        )

    fetch(0)
    barrier = pltpu.get_barrier_semaphore()
    for d in range(1, peers):
        other = lax.rem(me + d, peers)
        pl.semaphore_signal(
            barrier,
            inc=1,
            device_id=device(other // n_chan, lax.rem(other, n_chan)),
            device_id_type=MESH,
        )

    for at in range(1, len(places)):
        fetch(at)
    arrive(0)

    per = LANES // block
    slabs = channels // 8
    pieces = [(img, slab) for img in range(own_imgs) for slab in range(slabs)]
    packs = -(-len(pieces) // per)
    for dest in range(n_chan * split):
        rows = []
        for pack in range(packs):
            parts = []
            for img, slab in pieces[pack * per : (pack + 1) * per]:
                parts.append(images[dest * own_imgs + img, slab * 8 : slab * 8 + 8, :])
            while len(parts) < per:
                parts.append(jnp.zeros((8, block), f32))
            rows.append(jnp.concatenate(parts, axis=1))
        outbox[dest] = jnp.concatenate(rows, axis=0).astype(bf16)

    pl.semaphore_wait(barrier, peers - 1)
    for d in range(1, peers):
        other = lax.rem(me + d, peers)
        other_chan = lax.rem(other, n_chan)
        copy = pltpu.make_async_remote_copy(
            src_ref=outbox.at[paired(other_chan) * split + lax.rem(other // n_chan, split)],
            dst_ref=inbox.at[me],
            send_sem=send_sem,
            recv_sem=recv_sem,
            device_id=device(other // n_chan, other_chan),
            device_id_type=MESH,
        )
        copy.start()

    inbox[me] = outbox[work * split + mine]

    for where in range(1, count):
        arrive(where)
    shift_mid, gain_mid, diag_mid, third_bias_mid = [vecs_mid[k] for k in range(4)]
    shift_top, gain_top, diag_top, third_bias_top = [vecs_top[k] for k in range(4)]
    lower_mid, upper_mid = mats_in_mid.at[0], mats_in_mid.at[1]
    lower_top, upper_top = mats_in_top.at[0], mats_in_top.at[1]
    deep = w13_all.shape[1]
    w3_mid = [w13_all.at[s] for s in range(steps_mid)]
    w1_top = [w13_all.at[steps_mid + s] for s in range(steps_top)]
    w3_top = [
        w13_all.at[pl.ds(steps_mid + steps_top + 2 * s, 2)] for s in range(steps_top)
    ]
    half = channels // 2
    padded = up8(half)
    top_channels = 4 * half
    mats_mid = []
    for s in range(steps_mid):
        mats_mid.append(
            mixing(
                mix_mid.at[s],
                lower_mid[s],
                upper_mid[s],
                diag_mid[s : s + 1, :],
                gain_mid[s : s + 1, :],
                shift_mid[s : s + 1, :],
                None if s == 0 else pad_map(channels),
            )
        )
    mats_top = []
    for s in range(steps_top):
        mats_top.append(
            mixing(
                mix_top.at[s],
                lower_top[s],
                upper_top[s],
                diag_top[s : s + 1, :],
                gain_top[s : s + 1, :],
                shift_top[s : s + 1, :],
                squeeze_map(half, padded) if s == 0 else pad_map(top_channels),
            )
        )
    bias3_mid = [to_column(third_bias_mid[s : s + 1, :]) for s in range(steps_mid)]
    bias3_top = [to_column(third_bias_top[s : s + 1, :]) for s in range(steps_top)]
    for s in range(steps_mid):
        for tap in range(9):
            w = w1_raw[s, tap].astype(f32)
            if padded > half:
                w = jnp.concatenate([w, jnp.zeros((padded - half, w.shape[1]), f32)], axis=0)
            w1_mid[s, tap * padded : (tap + 1) * padded, :] = w.astype(bf16)
    const_mid = height * width * (jnp.sum(gain_mid) + jnp.sum(diag_mid))
    const_top = (height // 2) * (width // 2) * (jnp.sum(gain_top) + jnp.sum(diag_top))

    if peers > 1:
        drain(inbox, peers - 1, send_sem, recv_sem).wait_recv()

    cells = height * width
    n_mid = own_imgs * cells
    depth = cells // LANES
    own_rows = block // width
    columns = []
    letters = [inbox[source].astype(f32) for source in range(peers)]
    for img in range(own_imgs):
        for tile in range(depth):
            stack = []
            for slab in range(slabs):
                at = img * slabs + slab
                top = at // per * 8
                parts = []
                for row in range(tile, height, depth):
                    lo = (at % per) * block + row % own_rows * width
                    parts.append(letters[row // own_rows][top : top + 8, lo : lo + width])
                stack.append(join(parts))
            columns.append(jnp.concatenate(stack, axis=0))
    s_mid[0, :channels, :] = join(columns)

    strip = n_chan * block
    team = split * n_chan
    seat = mine * n_chan + c

    def share(ua):
        z_scr[...] = by_row(ua, width, cells)
        for to_row in range(split):
            for img in range(own_imgs):
                begin = pl.multiple_of(img * cells + (base + to_row) * strip, LANES)
                z_send[to_row, img] = z_scr[:, pl.ds(begin, strip)].astype(bf16)
        for d in range(1, team):
            other = lax.rem(seat + d, team)
            copy = pltpu.make_async_remote_copy(
                src_ref=z_send.at[other // n_chan],
                dst_ref=z_recv.at[seat],
                send_sem=z_send_sem,
                recv_sem=z_recv_sem,
                device_id=device(base + other // n_chan, lax.rem(other, n_chan)),
                device_id_type=MESH,
            )
            copy.start()
        z_recv[seat] = z_send[mine]

    def step(held_state, rows, table, mat, bias, w1, b1, w2, b2, w3, b3, width, chans, last=False):
        n = held_state.shape[1]
        area = n // own_imgs
        half_c = chans // 2
        hp = up8(half_c)
        spans = range(0, n, LANES)
        sums = [[None] * 4 for _ in spans]
        for j in range(chans):
            row = rows[j]
            for k, at in enumerate(spans):
                term = table[j] * held_state[row : row + 1, at : at + LANES]
                old = sums[k][j % 4]
                sums[k][j % 4] = term if old is None else old + term
        ua = join([(x[0] + x[1]) + (x[2] + x[3]) + table[chans] for x in sums])
        ub = jnp.dot(
            mat, held_state[: mat.shape[1], :], precision=FINE, preferred_element_type=f32
        )
        ub = ub + bias
        if last:
            share(ua)
        spread = spread_taps(ua, width, area).astype(bf16)
        size = min(CHUNK, n)
        for at in range(0, n, size):
            h1 = dot_tn(spread[:, at : at + size], w1)
            h1 = jnp.maximum(h1 + b1, 0.0).astype(bf16)
            h2 = jnp.dot(h1, w2[...], preferred_element_type=f32)
            h2 = jnp.maximum(h2 + b2, 0.0).astype(bf16)
            w3_now = w3[...].reshape(9 * chans, -1)
            y_scr[: 9 * chans, at : at + size] = dot_nt(w3_now, h2)
        out = gather_taps(y_scr, chans, n, width, area) + b3
        g = out[:hp] + 2.0
        t = out[half_c:]
        if hp > half_c:
            t = jnp.concatenate([t, jnp.zeros((hp - half_c, n), f32)], axis=0)
        e = jnp.exp(-jnp.abs(g))
        inv = 1.0 / (1.0 + e)
        gate = jnp.where(g >= 0, inv, e * inv)
        logs = jnp.minimum(g, 0.0) - jnp.log(1.0 + e)
        if hp > half_c:
            logs = jnp.where(iota((hp, n), 0) < half_c, logs, 0.0)
        return ua, (ub + t) * gate, logs

    padded_rows = [j if j < half else padded + j - half for j in range(channels)]
    score = None
    for s in range(steps_mid):
        ua, updated, logs = step(
            s_mid.at[s],
            list(range(channels)) if s == 0 else padded_rows,
            mix_mid.at[s],
            *mats_mid[s],
            w1_mid[s],
            first_bias_mid[s : s + 1, :].astype(f32),
            w2_all.at[s],
            second_bias_mid[s : s + 1, :],
            w3_mid[s],
            bias3_mid[s],
            width,
            channels,
            s == steps_mid - 1,
        )
        score = logs if score is None else score + logs
        if s < steps_mid - 1:
            s_mid[s + 1, :padded, :] = ua
            s_mid[s + 1, padded : 2 * padded, :] = updated
    score = score - 0.5 * ua * ua

    coarse_w = width // 2
    lane = iota((padded, LANES), 1)
    strip_at = lax.div(lane, coarse_w)
    corner = lax.div(strip_at, 2) * width + 2 * lax.rem(lane, coarse_w)
    even = lax.rem(strip_at, 2) == 0
    for img in range(own_imgs):
        tiles = tiles_of(updated[:, img * cells : (img + 1) * cells])
        for tile in range(depth // 4):
            for i in range(2):
                for j in range(2):
                    upper_half = jnp.take_along_axis(tiles[2 * tile + i], corner + j, axis=1)
                    lower_half = jnp.take_along_axis(
                        tiles[depth // 2 + 2 * tile + i], corner + j, axis=1
                    )
                    at = img * cells // 4 + tile * LANES
                    top = (2 * i + j) * padded
                    s_top[0, top : top + padded, at : at + LANES] = jnp.where(
                        even, upper_half, lower_half
                    )

    n_top = n_mid // 4
    squeezed_rows = [j % 4 * padded + j // 4 for j in range(top_channels)]
    top_half = top_channels // 2
    top_padded = up8(top_half)
    top_rows = [j if j < top_half else top_padded + j - top_half for j in range(top_channels)]
    score_top = None
    for s in range(steps_top):
        ua, updated, logs = step(
            s_top.at[s],
            squeezed_rows if s == 0 else top_rows,
            mix_top.at[s],
            *mats_top[s],
            w1_top[s][...],
            first_bias_top[s : s + 1, :].astype(f32),
            w2_all.at[steps_mid + s],
            second_bias_top[s : s + 1, :],
            w3_top[s],
            bias3_top[s],
            coarse_w,
            top_channels,
        )
        score_top = logs if score_top is None else score_top + logs
        if s < steps_top - 1:
            s_top[s + 1, :top_padded, :] = ua
            s_top[s + 1, top_padded : 2 * top_padded, :] = updated
    state = jnp.concatenate([ua, updated], axis=0)
    score_top = score_top - 0.5 * (ua * ua + updated * updated)

    top_cells = cells // 4
    own = top_cells // n_rows
    hp = up8(top_channels // 2)
    if hp * 2 > top_channels:
        state = jnp.concatenate([ua[: top_channels // 2], updated[: top_channels // 2]], axis=0)
    fixed = const_mid + const_top - 0.5 * log_two_pi * (half * cells + top_channels * top_cells)
    high = t_send.shape[2]
    folds = -(-top_channels // high)
    if folds * high > top_channels:
        filler = jnp.zeros((folds * high - top_channels, n_top), f32)
        state = jnp.concatenate([state, filler], axis=0)
    t_scr[...] = by_row(state, coarse_w, top_cells)
    for img in range(own_imgs):
        total = jnp.sum(score[:, img * cells : (img + 1) * cells])
        total = total + jnp.sum(score_top[:, img * top_cells : (img + 1) * top_cells])
        lik = jnp.full((high, own), (total + fixed) / (channels * cells), f32)
        coarse = lik.astype(bf16).astype(f32)
        lik = jnp.where(iota((high, own), 0) == 0, coarse, lik - coarse)
        for to_row in range(split):
            at = img * top_cells + (base + to_row) * own
            window = t_scr[:, img * top_cells : (img + 1) * top_cells]
            parts = []
            for row in range(n_rows):
                piece = window[:, row * own : (row + 1) * own]
                parts.append(
                    jnp.concatenate(
                        [piece[k * high : (k + 1) * high] for k in range(folds)] + [lik], axis=1
                    )
                )
            chosen = parts[to_row]
            for start in range(split, n_rows, split):
                chosen = jnp.where(base == start, parts[start + to_row], chosen)
            t_send[to_row, img] = chosen.astype(bf16)
    t_count = split if swap else split - 1
    for d in range(split - t_count, split):
        other = lax.rem(mine + d, split)
        copy = pltpu.make_async_remote_copy(
            src_ref=t_send.at[other],
            dst_ref=t_recv.at[mine],
            send_sem=t_send_sem,
            recv_sem=t_recv_sem,
            device_id=device(base + other, work),
            device_id_type=MESH,
        )
        copy.start()
    if not swap:
        t_recv[mine] = t_send[mine]

    if team > 1:
        drain(z_recv, team - 1, z_send_sem, z_recv_sem).wait_recv()
    for here in range(n_chan):

        @pl.when(c == here)
        def _():
            for source in range(n_chan):
                holder = source + 1 - 2 * (source % 2) if swap else source
                for img in range(group):
                    sender = img // own_imgs * n_chan + holder
                    at = (source * group + img) * half
                    mid_out[at : at + half, :] = z_recv[sender, img % own_imgs].astype(f32)[
                        :half, here * block : (here + 1) * block
                    ]

    if peers > 1:
        drain(inbox, peers - 1, send_sem, recv_sem).wait_send()
    if team > 1:
        drain(z_recv, team - 1, z_send_sem, z_recv_sem).wait_send()
    if t_count > 0:
        drain(t_recv, t_count, t_send_sem, t_recv_sem).wait()
    liks = []
    letters = []
    for img in range(group):
        letter = t_recv[img // own_imgs, img % own_imgs].astype(f32)
        letters.append(letter)
        lik = letter[:2, folds * own : folds * own + 1]
        liks.append(lik[:1] + lik[1:])
    flipped = jnp.transpose(jnp.concatenate(letters, axis=0))
    for img in range(group):
        for k in range(folds):
            size = min(high, top_channels - k * high)
            top_out[img, :, k * high : k * high + size] = flipped[
                k * own : (k + 1) * own, img * high : img * high + size
            ]
    lik_out[...] = jnp.concatenate(liks, axis=1)


def deliver(*refs):
    count = len(refs) // 2
    sems = refs[-1]
    copies = [
        pltpu.make_async_copy(refs[at], refs[count + at], sems.at[at]) for at in range(count)
    ]
    for copy in copies:
        copy.start()
    for copy in copies:
        copy.wait()


def body(sizes, images, *params):
    (
        shift_mid,
        gain_mid,
        lower_mid,
        upper_mid,
        diag_mid,
        first_mid,
        first_bias_mid,
        second_mid,
        second_bias_mid,
        third_mid,
        third_bias_mid,
        shift_top,
        gain_top,
        lower_top,
        upper_top,
        diag_top,
        first_top,
        first_bias_top,
        second_top,
        second_bias_top,
        third_top,
        third_bias_top,
    ) = params
    n_rows, n_chan = sizes
    n_imgs, channels, own_rows, width = images.shape
    peers = n_rows * n_chan
    height = own_rows * peers
    block = own_rows * width
    group = n_imgs // n_chan
    half = channels // 2
    padded = up8(half)
    steps_mid, hidden = first_bias_mid.shape
    steps_top, top_channels = shift_top.shape
    cells = height * width
    split = group if n_rows % group == 0 else 1
    own_imgs = group // split
    n_mid = own_imgs * cells
    packs = -(-(own_imgs * (channels // 8)) * block // LANES)
    strip = n_chan * block
    own = cells // 4 // n_rows
    high = -(-top_channels // max(1, LANES // own - 1) // 16) * 16
    folds = -(-top_channels // high)

    deep = 9 * channels
    w1_top = first_top.reshape(steps_top, deep, hidden)
    w3_mid = third_mid.transpose(0, 1, 3, 2).reshape(steps_mid, deep, hidden)
    w3_top = third_top.transpose(0, 1, 3, 2).reshape(2 * steps_top, deep, hidden)
    layout = (
        ((images.reshape(n_imgs, channels, block), None),),
        tuple((x, k) for k, x in enumerate((shift_mid, gain_mid, diag_mid, third_bias_mid))),
        tuple((x, k) for k, x in enumerate((shift_top, gain_top, diag_top, third_bias_top))),
        ((lower_mid, 0), (upper_mid, 1)),
        ((lower_top, 0), (upper_top, 1)),
        ((first_mid, None),),
        ((first_bias_mid, None),),
        ((first_bias_top, None),),
        ((second_bias_mid, None),),
        ((second_bias_top, None),),
        ((second_mid, 0), (second_top, steps_mid)),
        ((w3_mid, 0), (w1_top, steps_mid), (w3_top, steps_mid + steps_top)),
    )
    operands, places, stores = [], [], []
    for where, entry in enumerate(layout):
        first = entry[0][0]
        joined = where >= len(layout) - 2
        if joined:
            shape = (sum(x.shape[0] for x, _ in entry),) + first.shape[1:]
        elif entry[0][1] is None:
            shape = first.shape
        else:
            shape = (len(entry),) + first.shape
        stores.append(pltpu.VMEM(shape, first.dtype))
        for x, offset in entry:
            operands.append(x)
            places.append((where, offset, x.shape[0] if joined else None))
    vmem = pl.BlockSpec(memory_space=pltpu.VMEM)
    hbm = pl.BlockSpec(memory_space=pl.ANY)
    count = len(stores)
    results = [
        (n_imgs * half, block),
        (group, own, top_channels),
        (1, group),
    ]
    held = pl.pallas_call(
        functools.partial(kernel, (n_rows, n_chan, split, height, width, places, count)),
        out_shape=[pltpu.VMEM(x, f32) for x in results],
        in_specs=[hbm] * len(operands),
        out_specs=[vmem] * len(results),
        scratch_shapes=stores
        + [
            pltpu.VMEM((n_chan * split, packs * 8, LANES), bf16),
            pltpu.VMEM((peers, packs * 8, LANES), bf16),
            pltpu.VMEM((steps_mid, 9 * padded, hidden), bf16),
            pltpu.VMEM((steps_mid, channels + 1, padded, LANES), f32),
            pltpu.VMEM((steps_top, top_channels + 1, up8(top_channels // 2), LANES), f32),
            pltpu.VMEM((steps_mid, 2 * padded, n_mid), f32),
            pltpu.VMEM((steps_top, 4 * padded, n_mid // 4), f32),
            pltpu.VMEM((9 * top_channels, n_mid), f32),
            pltpu.VMEM((padded, n_mid), f32),
            pltpu.VMEM((split, own_imgs, padded, strip), bf16),
            pltpu.VMEM((split * n_chan, own_imgs, padded, strip), bf16),
            pltpu.VMEM((split, own_imgs, high, (folds + 1) * own), bf16),
            pltpu.VMEM((split, own_imgs, high, (folds + 1) * own), bf16),
            pltpu.VMEM((folds * high, n_mid // 4), f32),
            pltpu.SemaphoreType.DMA((count,)),
            pltpu.SemaphoreType.DMA((6,)),
        ],
        compiler_params=pltpu.CompilerParams(
            collective_id=0, has_side_effects=True, vmem_limit_bytes=56 * 1024 * 1024
        ),
        name="flow",
    )(*operands)
    mid, top, lik = pl.pallas_call(
        deliver,
        out_shape=[jax.ShapeDtypeStruct(x, f32) for x in results],
        in_specs=[vmem] * len(results),
        out_specs=[hbm] * len(results),
        scratch_shapes=[pltpu.SemaphoreType.DMA((len(results),))],
        name="deliver",
    )(*[pltpu.with_memory_space_constraint(x, pltpu.VMEM) for x in held])
    latent_mid = mid.reshape(n_imgs, half, own_rows, width)
    latent_top = top.reshape(group, -1, width // 2, top_channels).transpose(0, 3, 1, 2)
    return latent_mid, latent_top, lik.reshape(group)


def solution(mesh):
    sizes = (mesh.shape["rows"], mesh.shape["chan"])
    placed = (P("batch", None, ("rows", "chan"), None),) + (P(),) * 22
    return jax.shard_map(
        functools.partial(body, sizes),
        mesh=mesh,
        in_specs=placed,
        out_specs=(
            P("batch", None, ("rows", "chan"), None),
            P(("batch", "chan"), None, "rows", None),
            P(("batch", "chan")),
        ),
        check_vma=False,
    )
```

```python
import functools
import math

import jax
import jax.numpy as jnp
from jax import lax
from jax.experimental import pallas as pl
from jax.experimental.pallas import tpu as pltpu
from jax.sharding import PartitionSpec as P

MESH = pl.DeviceIdType.MESH
LANES = 128
CHUNK = 512
FINE = lax.Precision.HIGHEST
log_two_pi = math.log(2.0 * math.pi)
f32 = jnp.float32
bf16 = jnp.bfloat16


def up8(n):
    return -(-n // 8) * 8


def iota(shape, dim):
    return lax.broadcasted_iota(jnp.int32, shape, dim)


def dot_nt(a, b, precision=None):
    return lax.dot_general(
        a, b, (((1,), (1,)), ((), ())), preferred_element_type=f32, precision=precision
    )


def dot_tn(a, b):
    return lax.dot_general(a, b, (((0,), (0,)), ((), ())), preferred_element_type=f32)


def roll_back(x, amount):
    n = x.shape[1]
    amount = amount % n
    return x if amount == 0 else pltpu.roll(x, n - amount, 1)


def keep(x, ok):
    return jnp.where(ok, x, 0.0)


def tiles_of(x):
    return [x[:, at : at + LANES] for at in range(0, x.shape[1], LANES)]


def join(parts):
    return parts[0] if len(parts) == 1 else jnp.concatenate(parts, axis=1)


def shift(tile, dr, dc, width):
    if dr == 0 and dc == 0:
        return tile
    lane = iota((1, LANES), 1)
    col = lax.rem(lane, width)
    strip = lax.div(lane, width)
    ok = None
    if dc != 0:
        ok = col < width - 1 if dc > 0 else col >= 1
    if dr != 0:
        row_ok = strip < LANES // width - 1 if dr > 0 else strip >= 1
        ok = row_ok if ok is None else ok & row_ok
    return keep(roll_back(tile, dr * width + dc), ok)


def by_row(x, width, cells):
    depth = cells // LANES
    if depth == 1:
        return x
    parts = []
    for at in range(0, x.shape[1], cells):
        for row in range(cells // width):
            lo = at + row % depth * LANES + row // depth * width
            parts.append(x[:, lo : lo + width])
    return join(parts)


def spread_taps(q, width, cells):
    tiles = tiles_of(q)
    depth = cells // LANES
    taps = []
    inside = {dc: [shift(x, 0, dc, width) for x in tiles] for dc in (-1, 0, 1)}
    for dr in (-1, 0, 1):
        for dc in (-1, 0, 1):
            moved = []
            for k in range(len(tiles)):
                at = k % depth + dr
                if 0 <= at < depth:
                    moved.append(inside[dc][k + dr])
                else:
                    moved.append(shift(tiles[k + dr - dr * depth], dr, dc, width))
            taps.append(join(moved))
    return jnp.concatenate(taps, axis=0)


def gather_taps(y_ref, channels, n, width, cells):
    depth = cells // LANES

    def tap(dr, dc, k):
        top = ((dr + 1) * 3 + dc + 1) * channels
        return y_ref[top : top + channels, k * LANES : (k + 1) * LANES]

    sums = []
    for k in range(n // LANES):
        total = None
        for dc in (-1, 1, 0):
            part = None
            for dr in (-1, 0, 1):
                if 0 <= k % depth + dr < depth:
                    y = tap(dr, dc, k + dr)
                    part = y if part is None else part + y
                else:
                    y = shift(tap(dr, dc, k + dr - dr * depth), dr, dc, width)
                    total = y if total is None else total + y
            part = shift(part, 0, dc, width)
            total = part if total is None else total + part
        sums.append(total)
    return join(sums)


def mixing(table, lower, upper, diag_row, gain_row, shift_row, in_map):
    channels = lower.shape[0]
    half = channels // 2
    padded = up8(half)
    i = iota((channels, channels), 0)
    j = iota((channels, channels), 1)
    eye = jnp.where(i == j, 1.0, 0.0)
    low = jnp.where(i > j, lower, 0.0) + eye
    upp = (jnp.where(i < j, upper, 0.0) + eye * jnp.exp(diag_row)) * jnp.exp(gain_row)
    out_map = pad_map(channels)
    rows = jnp.dot(out_map, low, precision=FINE, preferred_element_type=f32)
    mat = jnp.dot(rows, upp, precision=FINE, preferred_element_type=f32)
    bias = jnp.sum(mat * shift_row, axis=1, keepdims=True)
    for j in range(channels):
        table[j] = jnp.broadcast_to(mat[:padded, j : j + 1], (padded, LANES))
    table[channels] = jnp.broadcast_to(bias[:padded], (padded, LANES))
    mat, bias = mat[padded:], bias[padded:]
    if in_map is not None:
        mat = dot_nt(mat, in_map, FINE)
    high = mat.astype(bf16).astype(f32)
    return jnp.concatenate([high, high, mat - high], axis=1).astype(bf16), bias


def halves(x):
    high = x.astype(bf16).astype(f32)
    return jnp.concatenate([high, x - high, high], axis=0).astype(bf16)


def pad_map(channels):
    half = channels // 2
    padded = up8(half)
    i = iota((2 * padded, channels), 0)
    j = iota((2 * padded, channels), 1)
    first = (j < half) & (i == j)
    second = (j >= half) & (i - padded == j - half)
    return jnp.where(first | second, 1.0, 0.0)


def squeeze_map(kept, padded):
    i = iota((4 * padded, 4 * kept), 0)
    j = iota((4 * padded, 4 * kept), 1)
    same = (lax.rem(i, padded) == lax.div(j, 4)) & (lax.div(i, padded) == lax.rem(j, 4))
    return jnp.where(same, 1.0, 0.0)


def to_column(row):
    n = row.shape[1]
    eye = iota((n, n), 0) == iota((n, n), 1)
    return jnp.sum(jnp.where(eye, row, 0.0), axis=1, keepdims=True)


def kernel(dims, *refs):
    n_rows, n_chan, split, height, width, places, count = dims
    sources, refs = refs[: len(places)], refs[len(places) :]
    (mid_out, top_out, lik_out), refs = refs[:3], refs[3:]
    held, refs = refs[:count], refs[count:]
    (
        images,
        vecs_mid,
        vecs_top,
        mats_in_mid,
        mats_in_top,
        w1_raw,
        first_bias_mid,
        first_bias_top,
        second_bias_mid,
        second_bias_top,
        w2_all,
        w13_all,
    ) = held
    (
        outbox,
        inbox,
        w1_mid,
        mix_mid,
        mix_top,
        s_mid,
        s_top,
        y_scr,
        z_scr,
        z_send,
        z_recv,
        t_send,
        t_recv,
        t_scr,
        sems,
    ) = refs
    send_sem, recv_sem, z_send_sem, z_recv_sem, t_send_sem, t_recv_sem = [
        sems.at[k] for k in range(6)
    ]
    n_imgs, channels, block = images.shape
    steps_mid = vecs_mid.shape[1]
    steps_top = vecs_top.shape[1]
    group = n_imgs // n_chan
    peers = n_rows * n_chan
    b = lax.axis_index("batch")
    r = lax.axis_index("rows")
    c = lax.axis_index("chan")
    me = r * n_chan + c
    mine = lax.rem(r, split)
    base = r - mine
    own_imgs = group // split
    swap = split > 1 and n_chan % 2 == 0

    def paired(chan):
        return chan + 1 - 2 * lax.rem(chan, 2) if swap else chan

    work = paired(c)

    def device(row, chan):
        return {"batch": b, "rows": row, "chan": chan}

    def drain(ref, total, send, recv):
        return pltpu.make_async_remote_copy(
            src_ref=ref.at[pl.ds(0, total)],
            dst_ref=ref.at[pl.ds(0, total)],
            send_sem=send,
            recv_sem=recv,
            device_id=device(r, c),
            device_id_type=MESH,
        )

    per = LANES // block
    slabs = channels // 8
    pieces = [(img, slab) for img in range(own_imgs) for slab in range(slabs)]
    packs = -(-len(pieces) // per)

    def gather_all(w_sem):
        def fetch(at):
            where, offset, extent = places[at]
            target = held[where] if offset is None else held[where].at[offset]
            if extent is not None:
                target = held[where].at[pl.ds(offset, extent)]
            pltpu.make_async_copy(sources[at], target, w_sem.at[where]).start()

        def arrive(where):
            pltpu.make_async_copy(held[where], held[where], w_sem.at[where]).wait()

        for img in range(n_imgs):
            pltpu.make_async_copy(sources[0].at[img], images.at[img], w_sem.at[0]).start()
        barrier = pltpu.get_barrier_semaphore()
        for d in range(1, peers):
            other = lax.rem(me + d, peers)
            pl.semaphore_signal(
                barrier,
                inc=1,
                device_id=device(other // n_chan, lax.rem(other, n_chan)),
                device_id_type=MESH,
            )

        for at in range(1, len(places)):
            fetch(at)
        arrive(0)

        for dest in range(n_chan * split):
            rows = []
            for pack in range(packs):
                parts = []
                for img, slab in pieces[pack * per : (pack + 1) * per]:
                    parts.append(images[dest * own_imgs + img, slab * 8 : slab * 8 + 8, :])
                while len(parts) < per:
                    parts.append(jnp.zeros((8, block), f32))
                rows.append(jnp.concatenate(parts, axis=1))
            outbox[dest] = jnp.concatenate(rows, axis=0).astype(bf16)

        pl.semaphore_wait(barrier, peers - 1)
        for d in range(1, peers):
            other = lax.rem(me + d, peers)
            other_chan = lax.rem(other, n_chan)
            copy = pltpu.make_async_remote_copy(
                src_ref=outbox.at[paired(other_chan) * split + lax.rem(other // n_chan, split)],
                dst_ref=inbox.at[me],
                send_sem=send_sem,
                recv_sem=recv_sem,
                device_id=device(other // n_chan, other_chan),
                device_id_type=MESH,
            )
            copy.start()

        inbox[me] = outbox[work * split + mine]

        for where in range(1, count):
            arrive(where)

    pl.run_scoped(gather_all, pltpu.SemaphoreType.DMA((count,)))
    shift_mid, gain_mid, diag_mid, third_bias_mid = [vecs_mid[k] for k in range(4)]
    shift_top, gain_top, diag_top, third_bias_top = [vecs_top[k] for k in range(4)]
    lower_mid, upper_mid = mats_in_mid.at[0], mats_in_mid.at[1]
    lower_top, upper_top = mats_in_top.at[0], mats_in_top.at[1]
    deep = w13_all.shape[1]
    w3_mid = [w13_all.at[s] for s in range(steps_mid)]
    w1_top = [w13_all.at[steps_mid + s] for s in range(steps_top)]
    w3_top = [
        w13_all.at[pl.ds(steps_mid + steps_top + 2 * s, 2)] for s in range(steps_top)
    ]
    half = channels // 2
    padded = up8(half)
    top_channels = 4 * half
    mats_mid = []
    for s in range(steps_mid):
        mats_mid.append(
            mixing(
                mix_mid.at[s],
                lower_mid[s],
                upper_mid[s],
                diag_mid[s : s + 1, :],
                gain_mid[s : s + 1, :],
                shift_mid[s : s + 1, :],
                None if s == 0 else pad_map(channels),
            )
        )
    mats_top = []
    for s in range(steps_top):
        mats_top.append(
            mixing(
                mix_top.at[s],
                lower_top[s],
                upper_top[s],
                diag_top[s : s + 1, :],
                gain_top[s : s + 1, :],
                shift_top[s : s + 1, :],
                squeeze_map(half, padded) if s == 0 else pad_map(top_channels),
            )
        )
    bias3_mid = [to_column(third_bias_mid[s : s + 1, :]) for s in range(steps_mid)]
    bias3_top = [to_column(third_bias_top[s : s + 1, :]) for s in range(steps_top)]
    for s in range(steps_mid):
        for tap in range(9):
            w = w1_raw[s, tap].astype(f32)
            if padded > half:
                w = jnp.concatenate([w, jnp.zeros((padded - half, w.shape[1]), f32)], axis=0)
            w1_mid[s, tap * padded : (tap + 1) * padded, :] = w.astype(bf16)
    def sum_all(x):
        return jnp.sum(jnp.sum(x, axis=0, keepdims=True), axis=1, keepdims=True)

    cells = height * width
    fixed = cells * sum_all(gain_mid + diag_mid) + cells // 4 * sum_all(gain_top + diag_top)
    fixed = fixed / (channels * cells) - 0.5 * log_two_pi

    if peers > 1:
        drain(inbox, peers - 1, send_sem, recv_sem).wait_recv()

    n_mid = own_imgs * cells
    depth = cells // LANES
    own_rows = block // width
    columns = []
    letters = [inbox[source].astype(f32) for source in range(peers)]
    for img in range(own_imgs):
        for tile in range(depth):
            stack = []
            for slab in range(slabs):
                at = img * slabs + slab
                top = at // per * 8
                parts = []
                for row in range(tile, height, depth):
                    lo = (at % per) * block + row % own_rows * width
                    parts.append(letters[row // own_rows][top : top + 8, lo : lo + width])
                stack.append(join(parts))
            columns.append(jnp.concatenate(stack, axis=0))
    s_mid[0, :channels, :] = join(columns)

    strip = n_chan * block
    team = split * n_chan
    seat = mine * n_chan + c

    def share(ua):
        z_scr[...] = by_row(ua, width, cells)
        for to_row in range(split):
            for img in range(own_imgs):
                begin = pl.multiple_of(img * cells + (base + to_row) * strip, LANES)
                z_send[to_row, img] = z_scr[:, pl.ds(begin, strip)].astype(bf16)
        for d in range(1, team):
            other = lax.rem(seat + d, team)
            copy = pltpu.make_async_remote_copy(
                src_ref=z_send.at[other // n_chan],
                dst_ref=z_recv.at[seat],
                send_sem=z_send_sem,
                recv_sem=z_recv_sem,
                device_id=device(base + other // n_chan, lax.rem(other, n_chan)),
                device_id_type=MESH,
            )
            copy.start()
        z_recv[seat] = z_send[mine]

    def blend(held_state, rows, table):
        sums = []
        for at in range(0, held_state.shape[1], LANES):
            parts = [table[len(rows)]]
            for j in range(len(rows)):
                term = table[j] * held_state[rows[j] : rows[j] + 1, at : at + LANES]
                if len(parts) < 4:
                    parts.append(term)
                else:
                    parts[j % 4] = parts[j % 4] + term
            while len(parts) > 1:
                parts = [sum(parts[x : x + 2][1:], parts[x]) for x in range(0, len(parts), 2)]
            sums.append(parts[0])
        return sums

    def step(held_state, rows, table, ahead, mat, bias, w1, b1, w2, b2, w3, b3, width, chans, last=False):
        n = held_state.shape[1]
        area = n // own_imgs
        half_c = chans // 2
        hp = up8(half_c)
        ua = join(blend(held_state, rows, table))
        if last:
            share(ua)
        spread = spread_taps(ua, width, area).astype(bf16)
        if ahead is not None:
            ahead[:hp, :] = ua
        source = halves(held_state[: mat.shape[1] // 3, :])
        size = min(CHUNK, n)
        for at in range(0, n, size):
            h1 = dot_tn(spread[:, at : at + size], w1)
            h1 = jnp.maximum(h1 + b1, 0.0).astype(bf16)
            h2 = jnp.dot(h1, w2[...], preferred_element_type=f32)
            h2 = jnp.maximum(h2 + b2, 0.0).astype(bf16)
            if at == 0:
                ub = jnp.dot(mat, source, preferred_element_type=f32) + bias
            w3_now = w3[...].reshape(9 * chans, -1)
            y_scr[: 9 * chans, at : at + size] = dot_nt(w3_now, h2)
        out = gather_taps(y_scr, chans, n, width, area) + b3
        g = out[:hp] + 2.0
        t = out[half_c:]
        if hp > half_c:
            t = jnp.concatenate([t, jnp.zeros((hp - half_c, n), f32)], axis=0)
        gate = 0.5 * jnp.tanh(0.5 * g) + 0.5
        updated = (ub + t) * gate
        if ahead is not None:
            ahead[hp : 2 * hp, :] = updated
        logs = jnp.minimum(g, 0.0) - jnp.log(1.0 + jnp.exp(-jnp.abs(g)))
        if hp > half_c:
            logs = jnp.where(iota((hp, n), 0) < half_c, logs, 0.0)
        return ua, updated, logs

    padded_rows = [j if j < half else padded + j - half for j in range(channels)]
    score = None
    for s in range(steps_mid):
        more = s < steps_mid - 1
        ua, updated, logs = step(
            s_mid.at[s],
            list(range(channels)) if s == 0 else padded_rows,
            mix_mid.at[s],
            s_mid.at[s + 1] if more else None,
            *mats_mid[s],
            w1_mid[s],
            first_bias_mid[s : s + 1, :].astype(f32),
            w2_all.at[s],
            second_bias_mid[s : s + 1, :],
            w3_mid[s],
            bias3_mid[s],
            width,
            channels,
            s == steps_mid - 1,
        )
        score = logs if score is None else score + logs
    score = score - 0.5 * ua * ua

    def fold(x):
        tiles = [t[at : at + 8] for t in tiles_of(x) for at in range(0, t.shape[0], 8)]
        return sum(tiles[1:], tiles[0])

    mid_sums = [fold(score[:, img * cells : (img + 1) * cells]) for img in range(own_imgs)]

    coarse_w = width // 2
    lane = iota((padded, LANES), 1)
    strip_at = lax.div(lane, coarse_w)
    corner = lax.div(strip_at, 2) * width + 2 * lax.rem(lane, coarse_w)
    even = lax.rem(strip_at, 2) == 0
    for img in range(own_imgs):
        tiles = tiles_of(updated[:, img * cells : (img + 1) * cells])
        for tile in range(depth // 4):
            for i in range(2):
                for j in range(2):
                    upper_half = jnp.take_along_axis(tiles[2 * tile + i], corner + j, axis=1)
                    lower_half = jnp.take_along_axis(
                        tiles[depth // 2 + 2 * tile + i], corner + j, axis=1
                    )
                    at = img * cells // 4 + tile * LANES
                    top = (2 * i + j) * padded
                    s_top[0, top : top + padded, at : at + LANES] = jnp.where(
                        even, upper_half, lower_half
                    )

    n_top = n_mid // 4
    squeezed_rows = [j % 4 * padded + j // 4 for j in range(top_channels)]
    top_half = top_channels // 2
    top_padded = up8(top_half)
    top_rows = [j if j < top_half else top_padded + j - top_half for j in range(top_channels)]
    score_top = None
    for s in range(steps_top):
        more = s < steps_top - 1
        ua, updated, logs = step(
            s_top.at[s],
            squeezed_rows if s == 0 else top_rows,
            mix_top.at[s],
            s_top.at[s + 1] if more else None,
            *mats_top[s],
            w1_top[s][...],
            first_bias_top[s : s + 1, :].astype(f32),
            w2_all.at[steps_mid + s],
            second_bias_top[s : s + 1, :],
            w3_top[s],
            bias3_top[s],
            coarse_w,
            top_channels,
        )
        score_top = logs if score_top is None else score_top + logs
    state = jnp.concatenate([ua, updated], axis=0)
    score_top = score_top - 0.5 * (ua * ua + updated * updated)

    top_cells = cells // 4
    own = top_cells // n_rows
    hp = up8(top_channels // 2)
    if hp * 2 > top_channels:
        state = jnp.concatenate([ua[: top_channels // 2], updated[: top_channels // 2]], axis=0)
    high = t_send.shape[2] - 16
    reach = t_send.shape[3]
    folds = -(-top_channels // high)
    if folds * high > top_channels:
        filler = jnp.zeros((folds * high - top_channels, n_top), f32)
        state = jnp.concatenate([state, filler], axis=0)
    t_scr[...] = by_row(state, coarse_w, top_cells)
    for img in range(own_imgs):
        total = mid_sums[img] + fold(score_top[:, img * top_cells : (img + 1) * top_cells])
        coarse = total.astype(bf16).astype(f32)
        lik = jnp.concatenate([coarse, total - coarse], axis=0)
        if reach > LANES:
            lik = jnp.concatenate([lik, jnp.zeros((16, reach - LANES), f32)], axis=1)
        for to_row in range(split):
            window = t_scr[:, img * top_cells : (img + 1) * top_cells]
            parts = []
            for row in range(n_rows):
                piece = window[:, row * own : (row + 1) * own]
                pieces = [piece[k * high : (k + 1) * high] for k in range(folds)]
                if reach > folds * own:
                    pieces.append(jnp.zeros((high, reach - folds * own), f32))
                parts.append(join(pieces))
            chosen = parts[to_row]
            for start in range(split, n_rows, split):
                chosen = jnp.where(base == start, parts[start + to_row], chosen)
            t_send[to_row, img, :high] = chosen.astype(bf16)
            t_send[to_row, img, high:] = lik.astype(bf16)
    t_count = split if swap else split - 1
    for d in range(split - t_count, split):
        other = lax.rem(mine + d, split)
        copy = pltpu.make_async_remote_copy(
            src_ref=t_send.at[other],
            dst_ref=t_recv.at[mine],
            send_sem=t_send_sem,
            recv_sem=t_recv_sem,
            device_id=device(base + other, work),
            device_id_type=MESH,
        )
        copy.start()
    if not swap:
        t_recv[mine] = t_send[mine]

    if team > 1:
        drain(z_recv, team - 1, z_send_sem, z_recv_sem).wait_recv()
    for here in range(n_chan):

        @pl.when(c == here)
        def _():
            for source in range(n_chan):
                holder = source + 1 - 2 * (source % 2) if swap else source
                for img in range(group):
                    sender = img // own_imgs * n_chan + holder
                    at = (source * group + img) * half
                    mid_out[at : at + half, :] = z_recv[sender, img % own_imgs].astype(f32)[
                        :half, here * block : (here + 1) * block
                    ]

    if peers > 1:
        drain(inbox, peers - 1, send_sem, recv_sem).wait_send()
    if team > 1:
        drain(z_recv, team - 1, z_send_sem, z_recv_sem).wait_send()
    if t_count > 0:
        drain(t_recv, t_count, t_send_sem, t_recv_sem).wait()
    liks = []
    letters = []
    for img in range(group):
        letter = t_recv[img // own_imgs, img % own_imgs].astype(f32)
        letters.append(letter[:high])
        lik = letter[high:, :LANES]
        lik = jnp.sum(jnp.sum(lik, axis=0, keepdims=True), axis=1, keepdims=True)
        liks.append(lik / (channels * cells) + fixed)
    flipped = jnp.transpose(jnp.concatenate(letters, axis=0))
    for img in range(group):
        for k in range(folds):
            size = min(high, top_channels - k * high)
            top_out[img, :, k * high : k * high + size] = flipped[
                k * own : (k + 1) * own, img * high : img * high + size
            ]
    lik_out[...] = jnp.concatenate(liks, axis=1)


def deliver(*refs):
    count = len(refs) // 2
    sems = refs[-1]
    copies = [
        pltpu.make_async_copy(refs[at], refs[count + at], sems.at[at]) for at in range(count)
    ]
    for copy in copies:
        copy.start()
    for copy in copies:
        copy.wait()


def body(sizes, images, *params):
    (
        shift_mid,
        gain_mid,
        lower_mid,
        upper_mid,
        diag_mid,
        first_mid,
        first_bias_mid,
        second_mid,
        second_bias_mid,
        third_mid,
        third_bias_mid,
        shift_top,
        gain_top,
        lower_top,
        upper_top,
        diag_top,
        first_top,
        first_bias_top,
        second_top,
        second_bias_top,
        third_top,
        third_bias_top,
    ) = params
    n_rows, n_chan = sizes
    n_imgs, channels, own_rows, width = images.shape
    peers = n_rows * n_chan
    height = own_rows * peers
    block = own_rows * width
    group = n_imgs // n_chan
    half = channels // 2
    padded = up8(half)
    steps_mid, hidden = first_bias_mid.shape
    steps_top, top_channels = shift_top.shape
    cells = height * width
    split = group if n_rows % group == 0 else 1
    own_imgs = group // split
    n_mid = own_imgs * cells
    packs = -(-(own_imgs * (channels // 8)) * block // LANES)
    strip = n_chan * block
    own = cells // 4 // n_rows
    high = -(-top_channels // max(1, LANES // own) // 16) * 16
    folds = -(-top_channels // high)

    deep = 9 * channels
    w1_top = first_top.reshape(steps_top, deep, hidden)
    w3_mid = third_mid.transpose(0, 1, 3, 2).reshape(steps_mid, deep, hidden)
    w3_top = third_top.transpose(0, 1, 3, 2).reshape(2 * steps_top, deep, hidden)
    layout = (
        ((images.reshape(n_imgs, channels, block), None),),
        tuple((x, k) for k, x in enumerate((shift_mid, gain_mid, diag_mid, third_bias_mid))),
        tuple((x, k) for k, x in enumerate((shift_top, gain_top, diag_top, third_bias_top))),
        ((lower_mid, 0), (upper_mid, 1)),
        ((lower_top, 0), (upper_top, 1)),
        ((first_mid, None),),
        ((first_bias_mid, None),),
        ((first_bias_top, None),),
        ((second_bias_mid, None),),
        ((second_bias_top, None),),
        ((second_mid, 0), (second_top, steps_mid)),
        ((w3_mid, 0), (w1_top, steps_mid), (w3_top, steps_mid + steps_top)),
    )
    operands, places, stores = [], [], []
    for where, entry in enumerate(layout):
        first = entry[0][0]
        joined = where >= len(layout) - 2
        if joined:
            shape = (sum(x.shape[0] for x, _ in entry),) + first.shape[1:]
        elif entry[0][1] is None:
            shape = first.shape
        else:
            shape = (len(entry),) + first.shape
        stores.append(pltpu.VMEM(shape, first.dtype))
        for x, offset in entry:
            operands.append(x)
            places.append((where, offset, x.shape[0] if joined else None))
    vmem = pl.BlockSpec(memory_space=pltpu.VMEM)
    hbm = pl.BlockSpec(memory_space=pl.ANY)
    count = len(stores)
    results = [
        (n_imgs * half, block),
        (group, own, top_channels),
        (1, group),
    ]
    held = pl.pallas_call(
        functools.partial(kernel, (n_rows, n_chan, split, height, width, places, count)),
        out_shape=[pltpu.VMEM(x, f32) for x in results],
        in_specs=[hbm] * len(operands),
        out_specs=[vmem] * len(results),
        scratch_shapes=stores
        + [
            pltpu.VMEM((n_chan * split, packs * 8, LANES), bf16),
            pltpu.VMEM((peers, packs * 8, LANES), bf16),
            pltpu.VMEM((steps_mid, 9 * padded, hidden), bf16),
            pltpu.VMEM((steps_mid, channels + 1, padded, LANES), f32),
            pltpu.VMEM((steps_top, top_channels + 1, up8(top_channels // 2), LANES), f32),
            pltpu.VMEM((steps_mid, 2 * padded, n_mid), f32),
            pltpu.VMEM((steps_top, 4 * padded, n_mid // 4), f32),
            pltpu.VMEM((9 * top_channels, n_mid), f32),
            pltpu.VMEM((padded, n_mid), f32),
            pltpu.VMEM((split, own_imgs, padded, strip), bf16),
            pltpu.VMEM((split * n_chan, own_imgs, padded, strip), bf16),
            pltpu.VMEM((split, own_imgs, high + 16, max(LANES, folds * own)), bf16),
            pltpu.VMEM((split, own_imgs, high + 16, max(LANES, folds * own)), bf16),
            pltpu.VMEM((folds * high, n_mid // 4), f32),
            pltpu.SemaphoreType.DMA((6,)),
        ],
        compiler_params=pltpu.CompilerParams(
            collective_id=0, has_side_effects=True, vmem_limit_bytes=56 * 1024 * 1024
        ),
        name="flow",
    )(*operands)
    mid, top, lik = pl.pallas_call(
        deliver,
        out_shape=[jax.ShapeDtypeStruct(x, f32) for x in results],
        in_specs=[vmem] * len(results),
        out_specs=[hbm] * len(results),
        scratch_shapes=[pltpu.SemaphoreType.DMA((len(results),))],
        name="deliver",
    )(*[pltpu.with_memory_space_constraint(x, pltpu.VMEM) for x in held])
    latent_mid = mid.reshape(n_imgs, half, own_rows, width)
    latent_top = top.reshape(group, -1, width // 2, top_channels).transpose(0, 3, 1, 2)
    return latent_mid, latent_top, lik.reshape(group)


def solution(mesh):
    sizes = (mesh.shape["rows"], mesh.shape["chan"])
    placed = (P("batch", None, ("rows", "chan"), None),) + (P(),) * 22
    return jax.shard_map(
        functools.partial(body, sizes),
        mesh=mesh,
        in_specs=placed,
        out_specs=(
            P("batch", None, ("rows", "chan"), None),
            P(("batch", "chan"), None, "rows", None),
            P(("batch", "chan")),
        ),
        check_vma=False,
    )
```
